32 devices in a mesh: dp: 8 (over z, y), mp: 4 (over x, core).
Axes of the slice: x: 2, y: 2, z: 4, core: 2. Of those that a mesh axis runs over, the one named last changes fastest.
Arguments:
- tokens: bfloat16 [2048, 4096], P('dp', 'mp'), may hold values from -6 to 6
- router_weight: bfloat16 [4096, 64], P('mp'), may hold values from -1 to 1
- valid_count: int32 [8], P('dp'), may hold values from 64 to 256, as said below
- expert_id: int32 [2048], P('dp'), may hold values from 0 to 63, as said below
- slot_id: int32 [2048], P('dp'), may hold values from 0 to 5
Outputs:
- gates: float32 [2048], P('dp')
- dispatched: bfloat16 [384, 8, 4096], P('dp', None, 'mp')
The draws below stay inside these ranges and needn't reach their ends.
Inputs may be any that keep to these rules, and one draw needn't show every extreme that they name: Group g's live tokens are its first valid_count[g] positions; the last group is full. Within one group no two positions share an expert and a slot. Flat slots expert_id * 6 + slot_id are held 48 in a row by one owner; one group's positions take at most 32 slots of any owner, and in every group some owner has 32 of its slots taken by live tokens.
All inputs are finite; a program needn't handle non-finite values.
Results may differ from the reference program's by a relative error of at most 0.001.
Values may be sent and summed in bfloat16 or wider, within the bound.
A program may use at most 64 MiB of HBM per device.

```python
import jax
import jax.numpy as jnp

D = 4096
E = 64
ITERS = 5
TOK_DEV = 256
CAP = 6
TOKENS = 2048
SEND = 32


def draw_valid_count(key, part):
    groups = TOKENS // TOK_DEV
    lowest = TOK_DEV // 4
    index = jnp.arange(groups, dtype=jnp.int32)
    rising = lowest + (TOK_DEV - lowest) * index // max(groups - 1, 1)
    jitter = jax.random.randint(jax.random.fold_in(key, 11), (groups,), 0, TOK_DEV // 8 + 1)
    counts = jnp.maximum(rising - jitter, lowest)
    return jnp.where(index == groups - 1, TOK_DEV, counts).astype(jnp.int32)


def slot_table(key):
    base_key = jax.random.fold_in(key, 7)
    groups = TOKENS // TOK_DEV
    block_size = E * CAP // groups
    most = SEND
    pool_size = groups * most

    def one_group(group_key):
        owner_keys = jax.random.split(jax.random.fold_in(group_key, 1), groups)

        def owner_pick(owner_key):
            return jax.random.permutation(owner_key, block_size)[:most].astype(jnp.int32)
        picks = jax.vmap(owner_pick)(owner_keys)
        owners = jnp.arange(groups, dtype=jnp.int32)
        flat = (owners[:, None] * block_size + picks).reshape(-1)
        front = jax.random.randint(jax.random.fold_in(group_key, 2), (), 0, groups)
        score = jax.random.permutation(jax.random.fold_in(group_key, 3), pool_size).astype(jnp.int32)
        owner_of = jnp.arange(pool_size, dtype=jnp.int32) // most
        score = jnp.where(owner_of == front, score - pool_size, score)
        order = jnp.argsort(score)
        return flat[order][:TOK_DEV].astype(jnp.int32)

    def group_key_of(number):
        return jax.random.fold_in(base_key, number + 100)
    group_keys = jax.vmap(group_key_of)(jnp.arange(groups, dtype=jnp.int32))
    return jax.vmap(one_group)(group_keys).reshape(-1)


def draw_expert_id(key, part):
    return (slot_table(key) // CAP).astype(jnp.int32)


def draw_slot_id(key, part):
    return (slot_table(key) % CAP).astype(jnp.int32)


def steps_of(stream_key, extent, cuts, least, top_value):
    def one(dim, shards_of):
        draws = jax.random.uniform(jax.random.fold_in(jax.random.fold_in(stream_key, 6), dim), (shards_of,), jnp.float32, least / len(cuts), top_value / len(cuts))
        return jnp.repeat(jnp.exp(draws), extent[dim] // shards_of).reshape((-1,) + (1,) * (len(extent) - dim - 1))

    loudness = one(*cuts[0])
    for cut in cuts[1:]:
        loudness = loudness * one(*cut)
    return loudness


def noise(stream_key, shape, scale, bound, cuts=(), held_as=jnp.bfloat16):
    result = jax.random.normal(stream_key, shape, jnp.float32) * scale
    if len(cuts) > 0:
        result = steps_of(stream_key, shape, cuts, -0.22, 0.18) * result
    return jnp.clip(result, min=-bound, max=bound).astype(held_as)


def setup_inputs(seed: int = 0) -> dict:
    key_of = jax.random.split(jax.random.key(seed), 6)
    tokens = noise(key_of[0], (TOKENS, D), 1.0, 6.0, ((0, 8), (1, 4)))
    router_weight = noise(key_of[1], (D, E), (4.0 * D ** -0.5), 1.0, ((0, 4),))
    valid_count = draw_valid_count(jax.random.fold_in(key_of[5], 71), 0)
    expert_id = draw_expert_id(jax.random.fold_in(key_of[5], 71), 0)
    slot_id = draw_slot_id(jax.random.fold_in(key_of[5], 71), 0)
    return dict(tokens=tokens, router_weight=router_weight, valid_count=valid_count, expert_id=expert_id, slot_id=slot_id)


def reference(tokens, router_weight, valid_count, expert_id, slot_id):
    logits = jnp.dot(tokens, router_weight, preferred_element_type=jnp.float32)
    affinity = jnp.exp(logits)
    groups = valid_count.shape[0]
    indices = jnp.arange(TOKENS, dtype=jnp.int32)
    position = indices % TOK_DEV
    group_of = indices // TOK_DEV
    live = position < valid_count[group_of]
    weight = live.astype(jnp.float32)
    total = jnp.sum(valid_count.astype(jnp.float32))
    col_scale = jnp.ones((E,), jnp.float32)
    row_scale = jnp.ones((TOKENS,), jnp.float32)
    for sweep in range(ITERS):
        row_scale = E / jnp.sum(affinity * col_scale[None, :], axis=1)
        column = jnp.sum(affinity * (weight * row_scale)[:, None], axis=0)
        col_scale = total / column
    chosen = expert_id[:, None] == jnp.arange(E, dtype=jnp.int32)[None, :]
    picked = jnp.sum(jnp.where(chosen, affinity * col_scale[None, :], 0.0), axis=1)
    gates = weight * row_scale * picked
    outside = E * CAP * groups
    target = jnp.where(live, (expert_id * CAP + slot_id) * groups + group_of, outside)
    buffer = jnp.zeros((outside, tokens.shape[1]), jnp.bfloat16).at[target].set(tokens, mode="drop")
    dispatched = buffer.reshape(E * CAP, groups, tokens.shape[1])
    return gates, dispatched
```

```python
import functools

import jax
import jax.numpy as jnp
from jax import lax
from jax.experimental import pallas as pl
from jax.experimental.pallas import tpu as pltpu
from jax.sharding import PartitionSpec as P

ITERS = 5
CAP = 6
MESH = pl.DeviceIdType.MESH
F32 = jnp.float32
BF16 = jnp.bfloat16


def iota(shape, dim):
    return lax.broadcasted_iota(jnp.int32, shape, dim)


def kernel(
    n_dp, n_mp, send, early,
    tokens_ref, weight_ref, count_ref, expert_ref, slot_ref,
    gates_ref, out_ref,
    part, part_in, aff, packed, packed_in, meta, meta_in, live,
    p2s, p2r, p3s, p3r, p4s, p4r, bs, br, ms, mr,
):
    rows = tokens_ref.shape[0]
    experts = weight_ref.shape[1]
    share = experts // n_mp
    owned = experts * CAP // n_dp
    lanes = n_dp * send
    i = lax.axis_index("dp")
    j = lax.axis_index("mp")
    few = n_dp <= 16

    def over(low, high, body):
        def step(k, carry):
            body(k)
            return carry
        lax.fori_loop(low, high, step, 0, unroll=few)

    def dp_peer(k):
        return lax.rem(i + k, n_dp)

    def mp_peer(k):
        return lax.rem(j + k, n_mp)

    barrier = pltpu.get_barrier_semaphore()
    over(1, n_dp, lambda k: pl.semaphore_signal(
        barrier, inc=1, device_id={"dp": dp_peer(k)}, device_id_type=MESH))
    for k in range(1, n_mp):
        pl.semaphore_signal(barrier, inc=1, device_id={"mp": mp_peer(k)}, device_id_type=MESH)

    tokens = tokens_ref[...]
    part[...] = lax.dot_general(
        weight_ref[...], tokens, (((0,), (1,)), ((), ())), preferred_element_type=F32)

    count = count_ref[0]
    target = expert_ref[...] * CAP + slot_ref[...]
    first = iota((n_dp, rows), 0) * owned
    offset = target - first
    mine = (offset >= 0) & (offset < owned)
    mine_f = mine.astype(F32)
    before = (iota((rows, rows), 0) < iota((rows, rows), 1)).astype(F32).astype(BF16)
    ranks = jnp.dot(mine_f.astype(BF16), before, preferred_element_type=F32)
    rank = jnp.sum(ranks * mine_f, axis=0, keepdims=True)
    base = jnp.sum(iota((n_dp, rows), 0).astype(F32) * mine_f, axis=0, keepdims=True)
    is_live = iota((1, rows), 1) < count
    value = jnp.where(mine & is_live, offset + 1, 0).astype(F32)
    column = (rank + (i * send).astype(F32)).astype(jnp.int32)
    spread = (iota((lanes, rows), 0) == column).astype(F32).astype(BF16)
    table = lax.dot_general(
        value.astype(BF16), spread, (((1,), (1,)), ((), ())), preferred_element_type=F32)
    for o in range(n_dp):
        meta[o, :, :lanes] = table[o:o + 1, :]
        meta[o, :, lanes:] = jnp.full((1, 128), count.astype(F32), F32)
    place = jnp.where(is_live, (base * send + rank).astype(jnp.int32), -1)
    chunk = min(lanes, 256)
    for top in range(0, lanes, chunk):
        pick = (iota((chunk, rows), 0) + top == place).astype(F32).astype(BF16)
        packed[top:top + chunk, :] = jnp.dot(
            pick, tokens, preferred_element_type=F32).astype(BF16)

    pl.semaphore_wait(barrier, n_dp + n_mp - 2)

    def span(index, size):
        return pl.ds(pl.multiple_of(index * size, size), size)

    def p2(peer, at):
        return pltpu.make_async_remote_copy(
            src_ref=part.at[span(peer, share)], dst_ref=part_in.at[at],
            send_sem=p2s.at[peer], recv_sem=p2r.at[at],
            device_id={"mp": peer}, device_id_type=MESH)

    def p3(peer, at):
        block = aff.at[at, span(j, share)]
        return pltpu.make_async_remote_copy(
            src_ref=block, dst_ref=block, send_sem=p3s.at[peer], recv_sem=p3r.at[at],
            device_id={"dp": peer}, device_id_type=MESH)

    def p4(peer, at, group):
        block = aff.at[group, span(at, share)]
        return pltpu.make_async_remote_copy(
            src_ref=block, dst_ref=block,
            send_sem=p4s.at[peer, group], recv_sem=p4r.at[at, group],
            device_id={"mp": peer}, device_id_type=MESH)

    def bulk(peer, at):
        return pltpu.make_async_remote_copy(
            src_ref=packed.at[span(peer, send)], dst_ref=packed_in.at[span(at, send)],
            send_sem=bs.at[peer], recv_sem=br.at[at],
            device_id={"dp": peer}, device_id_type=MESH)

    def note(peer, at):
        return pltpu.make_async_remote_copy(
            src_ref=meta.at[peer], dst_ref=meta_in.at[at],
            send_sem=ms.at[peer], recv_sem=mr.at[at],
            device_id={"dp": peer}, device_id_type=MESH)

    for k in range(1, n_mp):
        p2(mp_peer(k), j).start()
    over(1, n_dp, lambda k: note(dp_peer(k), i).start())
    split = min(early + 1, n_dp)
    over(1, split, lambda k: bulk(dp_peer(k), i).start())

    total_logits = part[span(j, share), :]
    for k in range(1, n_mp):
        src = mp_peer(k)
        p2(src, src).wait_recv()
        total_logits = total_logits + part_in[src]
    aff[i, span(j, share), :] = jnp.exp(total_logits)
    over(1, n_dp, lambda k: p3(dp_peer(k), i).start())
    for k in range(1, n_mp):
        p4(mp_peer(k), j, i).start()
    over(split, n_dp, lambda k: bulk(dp_peer(k), i).start())

    packed_in[span(i, send), :] = packed[span(i, send), :]
    meta_in[i] = meta[i]

    def forward(k):
        src = lax.rem(i + n_dp - k, n_dp)
        p3(src, src).wait_recv()
        for m in range(1, n_mp):
            p4(mp_peer(m), j, src).start()
    over(1, n_dp, forward)

    over(1, n_dp, lambda k: note(dp_peer(k), dp_peer(k)).wait_recv())
    where_to = jnp.zeros((1, lanes), F32)
    total = jnp.zeros((1, 1), F32)
    for g in range(n_dp):
        value = meta_in[g, :, :lanes]
        where_to = where_to + jnp.where(value > 0, (value - 1) * n_dp + (g + 1), 0.0)
        held = meta_in[g, :, lanes:lanes + 1]
        total = total + held
        live[g] = (iota((1, rows), 1).astype(F32) < held).astype(F32)
    place_in = (where_to - 1).astype(jnp.int32)
    unpack = (iota((owned * n_dp, lanes), 0) == place_in).astype(F32).astype(BF16)

    def landed(k):
        for m in range(1, n_mp):
            src = mp_peer(m)
            p4(src, src, dp_peer(k)).wait_recv()
    over(0, n_dp, landed)

    col_scale = jnp.ones((experts, 1), F32)
    last = col_scale
    for sweep in range(ITERS):
        last = col_scale
        scale = jnp.broadcast_to(last, (experts, rows))

        def add_group(g, acc, scale=scale):
            block = aff[g]
            row_scale = experts / jnp.sum(block * scale, axis=0, keepdims=True)
            return acc + block * (live[g] * row_scale)
        acc = lax.fori_loop(0, n_dp, add_group, jnp.zeros((experts, rows), F32), unroll=few)
        col_scale = total / jnp.sum(acc, axis=1, keepdims=True)

    block = aff[i]
    row_scale = experts / jnp.sum(block * last, axis=0, keepdims=True)
    chosen = expert_ref[...] == iota((experts, rows), 0)
    picked = jnp.sum(jnp.where(chosen, block * col_scale, 0.0), axis=0, keepdims=True)
    gates_ref[...] = live[i] * row_scale * picked

    over(1, n_dp, lambda k: bulk(dp_peer(k), dp_peer(k)).wait_recv())
    out_ref[...] = jnp.dot(unpack, packed_in[...], preferred_element_type=F32).astype(BF16)

    for k in range(1, n_mp):
        p2(mp_peer(k), j).wait_send()

    def drained(k):
        p3(dp_peer(k), i).wait_send()
        bulk(dp_peer(k), i).wait_send()
        note(dp_peer(k), i).wait_send()
    over(1, n_dp, drained)

    def forwarded(k):
        for m in range(1, n_mp):
            p4(mp_peer(m), j, dp_peer(k)).wait_send()
    over(0, n_dp, forwarded)


EARLY = 0


def solution(mesh):
    n_dp, n_mp = mesh.shape["dp"], mesh.shape["mp"]

    def local(tokens, router_weight, valid_count, expert_id, slot_id):
        rows, width = tokens.shape
        experts = router_weight.shape[1]
        share = experts // n_mp
        send = -(-(rows // n_dp) // 16) * 16
        lanes = n_dp * send
        slots = experts * CAP // n_dp
        vmem = pl.BlockSpec(memory_space=pltpu.VMEM)
        dma = pltpu.SemaphoreType.DMA
        gates, out = pl.pallas_call(
            functools.partial(kernel, n_dp, n_mp, send, EARLY),
            out_shape=(
                jax.ShapeDtypeStruct((1, rows), F32),
                jax.ShapeDtypeStruct((slots * n_dp, width), BF16),
            ),
            in_specs=[vmem, vmem, pl.BlockSpec(memory_space=pltpu.SMEM), vmem, vmem],
            out_specs=(vmem, vmem),
            scratch_shapes=[
                pltpu.VMEM((experts, rows), F32),
                pltpu.VMEM((n_mp, share, rows), F32),
                pltpu.VMEM((n_dp, experts, rows), F32),
                pltpu.VMEM((lanes, width), BF16),
                pltpu.VMEM((lanes, width), BF16),
                pltpu.VMEM((n_dp, 1, lanes + 128), F32),
                pltpu.VMEM((n_dp, 1, lanes + 128), F32),
                pltpu.VMEM((n_dp, 1, rows), F32),
                dma((n_mp,)), dma((n_mp,)), dma((n_dp,)), dma((n_dp,)),
                dma((n_mp, n_dp)), dma((n_mp, n_dp)),
                dma((n_dp,)), dma((n_dp,)), dma((n_dp,)), dma((n_dp,)),
            ],
            compiler_params=pltpu.CompilerParams(
                collective_id=0, has_side_effects=True, vmem_limit_bytes=60 * 1024 * 1024),
        )(tokens, router_weight, valid_count, expert_id.reshape(1, rows), slot_id.reshape(1, rows))
        return gates.reshape(rows), out.reshape(slots, n_dp, width)

    placed = (P("dp", "mp"), P("mp", None), P("dp"), P("dp"), P("dp"))
    return jax.shard_map(
        local, mesh=mesh, in_specs=placed, out_specs=(P("dp"), P("dp", None, "mp")), check_vma=False
    )
```

```python
import functools

import jax
import jax.numpy as jnp
from jax import lax
from jax.experimental import pallas as pl
from jax.experimental.pallas import tpu as pltpu
from jax.sharding import PartitionSpec as P

ITERS = 5
CAP = 6
MESH = pl.DeviceIdType.MESH
F32 = jnp.float32
BF16 = jnp.bfloat16


def iota(shape, dim):
    return lax.broadcasted_iota(jnp.int32, shape, dim)


def kernel(
    n_dp, n_mp, send, early,
    tokens_hbm, weight_hbm, count_ref, expert_hbm, slot_hbm,
    gates_ref, place_ref, packed_in,
    tokens_ref, weight_ref, expert_ref, slot_ref, part, part_in, aff, packed, meta, meta_in, live,
    own, p2s, p2r, p3s, p3r, p4s, p4r, bs, br, ms, mr,
):
    rows = tokens_ref.shape[0]
    experts = weight_ref.shape[0]
    share = experts // n_mp
    owned = experts * CAP // n_dp
    lanes = n_dp * send
    i = lax.axis_index("dp")
    j = lax.axis_index("mp")
    few = n_dp <= 16

    def over(low, high, body):
        def step(k, carry):
            body(k)
            return carry
        lax.fori_loop(low, high, step, 0, unroll=few)

    def dp_peer(k):
        return lax.rem(i + k, n_dp)

    def mp_peer(k):
        return lax.rem(j + k, n_mp)

    fetches = [
        pltpu.make_async_copy(src, dst, own.at[n])
        for n, (src, dst) in enumerate((
            (tokens_hbm, tokens_ref), (weight_hbm, weight_ref),
            (expert_hbm, expert_ref), (slot_hbm, slot_ref)))
    ]
    for fetch in fetches:
        fetch.start()

    barrier = pltpu.get_barrier_semaphore()
    over(1, n_dp, lambda k: pl.semaphore_signal(
        barrier, inc=1, device_id={"dp": dp_peer(k)}, device_id_type=MESH))
    for k in range(1, n_mp):
        pl.semaphore_signal(barrier, inc=1, device_id={"mp": mp_peer(k)}, device_id_type=MESH)

    fetches[2].wait()
    fetches[3].wait()
    count = count_ref[0]
    target = expert_ref[...] * CAP + slot_ref[...]
    first = iota((n_dp, rows), 0) * owned
    offset = target - first
    mine = (offset >= 0) & (offset < owned)
    mine_f = mine.astype(F32)
    before = (iota((rows, rows), 0) < iota((rows, rows), 1)).astype(F32).astype(BF16)
    ranks = jnp.dot(mine_f.astype(BF16), before, preferred_element_type=F32)
    rank = jnp.sum(ranks * mine_f, axis=0, keepdims=True)
    base = jnp.sum(iota((n_dp, rows), 0).astype(F32) * mine_f, axis=0, keepdims=True)
    is_live = iota((1, rows), 1) < count
    value = jnp.where(mine & is_live, offset + 1, 0).astype(F32)
    column = (rank + (i * send).astype(F32)).astype(jnp.int32)
    spread = (iota((lanes, rows), 0) == column).astype(F32).astype(BF16)
    table = lax.dot_general(
        value.astype(BF16), spread, (((1,), (1,)), ((), ())), preferred_element_type=F32)
    for o in range(n_dp):
        meta[o, :, :lanes] = table[o:o + 1, :]
        meta[o, :, lanes:] = jnp.full((1, 128), count.astype(F32), F32)
    place = jnp.where(is_live, (base * send + rank).astype(jnp.int32), -1)

    fetches[0].wait()
    fetches[1].wait()
    tokens = tokens_ref[...]
    part[...] = lax.dot_general(
        weight_ref[...], tokens, (((1,), (1,)), ((), ())), preferred_element_type=F32)

    chunk = min(lanes, 256)
    for top in range(0, lanes, chunk):
        pick = (iota((chunk, rows), 0) + top == place).astype(F32).astype(BF16)
        packed[top:top + chunk, :] = jnp.dot(
            pick, tokens, preferred_element_type=F32).astype(BF16)

    pl.semaphore_wait(barrier, n_dp + n_mp - 2)

    def span(index, size):
        return pl.ds(pl.multiple_of(index * size, size), size)

    def p2(peer, at):
        return pltpu.make_async_remote_copy(
            src_ref=part.at[span(peer, share)], dst_ref=part_in.at[at],
            send_sem=p2s.at[peer], recv_sem=p2r.at[at],
            device_id={"mp": peer}, device_id_type=MESH)

    def p3(peer, at):
        block = aff.at[at, span(j, share)]
        return pltpu.make_async_remote_copy(
            src_ref=block, dst_ref=block, send_sem=p3s.at[peer], recv_sem=p3r.at[at],
            device_id={"dp": peer}, device_id_type=MESH)

    pair = j + 1 - 2 * lax.rem(j, 2)

    def direct():
        return [lax.rem(j + 2 * m, n_mp) for m in range(1, n_mp // 2)]

    def p4(peer, at, group, lane=None):
        block = aff.at[group, span(at, share)]
        lane = peer if lane is None else lane
        return pltpu.make_async_remote_copy(
            src_ref=block, dst_ref=block,
            send_sem=p4s.at[lane, group], recv_sem=p4r.at[at, group],
            device_id={"mp": peer}, device_id_type=MESH)

    def bulk(peer, at):
        return pltpu.make_async_remote_copy(
            src_ref=packed.at[span(peer, send)], dst_ref=packed_in.at[span(at, send)],
            send_sem=bs.at[peer], recv_sem=br.at[at],
            device_id={"dp": peer}, device_id_type=MESH)

    def note(peer, at):
        return pltpu.make_async_remote_copy(
            src_ref=meta.at[peer], dst_ref=meta_in.at[at],
            send_sem=ms.at[peer], recv_sem=mr.at[at],
            device_id={"dp": peer}, device_id_type=MESH)

    for k in range(1, n_mp):
        p2(mp_peer(k), j).start()

    over(1, n_dp, lambda k: note(dp_peer(k), i).start())
    split = min(early + 1, n_dp)
    over(1, split, lambda k: bulk(dp_peer(k), i).start())

    total_logits = part[span(j, share), :]
    for k in range(1, n_mp):
        src = mp_peer(k)
        p2(src, src).wait_recv()
        total_logits = total_logits + part_in[src]
    aff[i, span(j, share), :] = jnp.exp(total_logits)
    over(1, n_dp, lambda k: p3(dp_peer(k), i).start())
    for peer in direct() + [pair]:
        p4(peer, j, i).start()
    over(split, n_dp, lambda k: bulk(dp_peer(k), i).start())

    keep = pltpu.make_async_copy(
        packed.at[span(i, send)], packed_in.at[span(i, send)], own.at[4])
    keep.start()
    meta_in[i] = meta[i]

    def forward(k):
        src = lax.rem(i + n_dp - k, n_dp)
        p3(src, src).wait_recv()
        for peer in direct() + [pair]:
            p4(peer, j, src).start()
    over(1, n_dp, forward)

    def across(peer):
        return peer + 1 - 2 * lax.rem(peer, 2)

    def relay(k):
        group = lax.rem(i + n_dp - k, n_dp)
        for src in direct():
            p4(src, src, group).wait_recv()
            p4(pair, src, group, across(src)).start()
    over(0, n_dp, relay)

    over(1, n_dp, lambda k: note(dp_peer(k), dp_peer(k)).wait_recv())
    where_to = jnp.zeros((1, lanes), F32)
    total = jnp.zeros((1, 1), F32)
    for g in range(n_dp):
        value = meta_in[g, :, :lanes]
        where_to = where_to + jnp.where(value > 0, (value - 1) * n_dp + (g + 1), 0.0)
        held = meta_in[g, :, lanes:lanes + 1]
        total = total + held
        live[g] = (iota((1, rows), 1).astype(F32) < held).astype(F32)
    place_ref[...] = (where_to - 1).astype(jnp.int32)

    def landed(k):
        for src in [pair] + [across(peer) for peer in direct()]:
            p4(pair, src, dp_peer(k)).wait_recv()
    over(0, n_dp, landed)

    col_scale = jnp.ones((experts, 1), F32)
    last = col_scale
    for sweep in range(ITERS):
        last = col_scale
        scale = jnp.broadcast_to(last, (experts, rows))

        def add_group(g, acc, scale=scale):
            block = aff[g]
            row_scale = experts / jnp.sum(block * scale, axis=0, keepdims=True)
            return acc + block * (live[g] * row_scale)
        acc = lax.fori_loop(0, n_dp, add_group, jnp.zeros((experts, rows), F32), unroll=few)
        col_scale = total / jnp.sum(acc, axis=1, keepdims=True)

    block = aff[i]
    row_scale = experts / jnp.sum(block * last, axis=0, keepdims=True)
    chosen = expert_ref[...] == iota((experts, rows), 0)
    picked = jnp.sum(jnp.where(chosen, block * col_scale, 0.0), axis=0, keepdims=True)
    gates_ref[...] = live[i] * row_scale * picked

    over(1, n_dp, lambda k: bulk(dp_peer(k), dp_peer(k)).wait_recv())
    keep.wait()

    for k in range(1, n_mp):
        p2(mp_peer(k), j).wait_send()

    def drained(k):
        p3(dp_peer(k), i).wait_send()
        bulk(dp_peer(k), i).wait_send()
        note(dp_peer(k), i).wait_send()
    over(1, n_dp, drained)

    def forwarded(k):
        for peer in direct() + [pair]:
            p4(peer, j, dp_peer(k)).wait_send()
        for src in direct():
            p4(pair, src, dp_peer(k), across(src)).wait_send()
    over(0, n_dp, forwarded)


def unpack(chunk, gates_in, place_ref, packed_ref, gates_ref, out_ref):
    gates_ref[...] = gates_in[...]
    at = iota((chunk, packed_ref.shape[0]), 0) + pl.program_id(0) * chunk
    pick = (at == place_ref[...]).astype(F32).astype(BF16)
    out_ref[...] = jnp.dot(pick, packed_ref[...], preferred_element_type=F32).astype(BF16)


EARLY = 2
CHUNK = 192
VMEM = 67043328
ROOM = 64
SMALL = 16 * 1024 * 1024


def solution(mesh):
    n_dp, n_mp = mesh.shape["dp"], mesh.shape["mp"]

    def local(tokens, router_weight, valid_count, expert_id, slot_id):
        rows, width = tokens.shape
        experts = router_weight.shape[1]
        share = experts // n_mp
        send = -(-(rows // n_dp) // 16) * 16
        lanes = n_dp * send
        slots = experts * CAP // n_dp
        total = slots * n_dp
        chunk = max(c for c in range(16, CHUNK + 1, 16) if total % c == 0)
        limit = VMEM - lanes * width * 2 - ROOM * 1024
        hbm = pl.BlockSpec(memory_space=pltpu.HBM)
        anywhere = pl.BlockSpec(memory_space=pl.ANY)
        vmem = pl.BlockSpec(memory_space=pltpu.VMEM)
        dma = pltpu.SemaphoreType.DMA
        gates, place, packed = pl.pallas_call(
            functools.partial(kernel, n_dp, n_mp, send, EARLY),
            out_shape=(
                pltpu.VMEM((1, rows), F32),
                pltpu.VMEM((1, lanes), jnp.int32),
                pltpu.VMEM((lanes, width), BF16),
            ),
            in_specs=[hbm, hbm, pl.BlockSpec(memory_space=pltpu.SMEM), hbm, hbm],
            out_specs=(vmem, vmem, anywhere),
            scratch_shapes=[
                pltpu.VMEM((rows, width), BF16),
                pltpu.VMEM((experts, width), BF16),
                pltpu.VMEM((1, rows), jnp.int32),
                pltpu.VMEM((1, rows), jnp.int32),
                pltpu.VMEM((experts, rows), F32),
                pltpu.VMEM((n_mp, share, rows), F32),
                pltpu.VMEM((n_dp, experts, rows), F32),
                pltpu.VMEM((lanes, width), BF16),
                pltpu.VMEM((n_dp, 1, lanes + 128), F32),
                pltpu.VMEM((n_dp, 1, lanes + 128), F32),
                pltpu.VMEM((n_dp, 1, rows), F32),
                dma((5,)), dma((n_mp,)), dma((n_mp,)), dma((n_dp,)), dma((n_dp,)),
                dma((n_mp, n_dp)), dma((n_mp, n_dp)),
                dma((n_dp,)), dma((n_dp,)), dma((n_dp,)), dma((n_dp,)),
            ],
            compiler_params=pltpu.CompilerParams(
                collective_id=0, has_side_effects=True, vmem_limit_bytes=limit),
        )(tokens, router_weight.T, valid_count, expert_id.reshape(1, rows), slot_id.reshape(1, rows))
        whole = lambda b: (0, 0)
        gates, out = pl.pallas_call(
            functools.partial(unpack, chunk),
            grid=(total // chunk,),
            out_shape=(
                jax.ShapeDtypeStruct((1, rows), F32),
                jax.ShapeDtypeStruct((total, width), BF16),
            ),
            in_specs=[
                pl.BlockSpec((1, rows), whole), pl.BlockSpec((1, lanes), whole), vmem],
            out_specs=(
                pl.BlockSpec((1, rows), whole), pl.BlockSpec((chunk, width), lambda b: (b, 0))),
            compiler_params=pltpu.CompilerParams(vmem_limit_bytes=SMALL),
        )(gates, place, packed)
        return gates.reshape(rows), out.reshape(slots, n_dp, width)

    placed = (P("dp", "mp"), P("mp", None), P("dp"), P("dp"), P("dp"))
    return jax.shard_map(
        local, mesh=mesh, in_specs=placed, out_specs=(P("dp"), P("dp", None, "mp")), check_vma=False
    )
```

```python
import functools

import jax
import jax.numpy as jnp
from jax import lax
from jax.experimental import pallas as pl
from jax.experimental.pallas import tpu as pltpu
from jax.sharding import PartitionSpec as P

ITERS = 5
CAP = 6
MESH = pl.DeviceIdType.MESH
F32 = jnp.float32
BF16 = jnp.bfloat16


def iota(shape, dim):
    return lax.broadcasted_iota(jnp.int32, shape, dim)


def kernel(
    n_dp, n_mp, send, early,
    tokens_hbm, weight_hbm, count_ref, expert_hbm, slot_hbm,
    gates_ref, place_ref, packed_in,
    tokens_ref, weight_ref, expert_ref, slot_ref, part, part_in, aff, packed, meta, meta_in, live,
    own, p2s, p2r, p3s, p3r, p4s, p4r, bs, br, ms, mr,
):
    rows = tokens_ref.shape[0]
    experts = weight_ref.shape[0]
    share = experts // n_mp
    owned = experts * CAP // n_dp
    lanes = n_dp * send
    i = lax.axis_index("dp")
    j = lax.axis_index("mp")
    few = n_dp <= 16

    def over(low, high, body):
        def step(k, carry):
            body(k)
            return carry
        lax.fori_loop(low, high, step, 0, unroll=few)

    def dp_peer(k):
        return lax.rem(i + k, n_dp)

    def mp_peer(k):
        return lax.rem(j + k, n_mp)

    fetches = [
        pltpu.make_async_copy(src, dst, own.at[n])
        for n, (src, dst) in enumerate((
            (tokens_hbm, tokens_ref), (weight_hbm, weight_ref),
            (expert_hbm, expert_ref), (slot_hbm, slot_ref)))
    ]
    for fetch in fetches:
        fetch.start()

    barrier = pltpu.get_barrier_semaphore()
    over(1, n_dp, lambda k: pl.semaphore_signal(
        barrier, inc=1, device_id={"dp": dp_peer(k)}, device_id_type=MESH))
    for k in range(1, n_mp):
        pl.semaphore_signal(barrier, inc=1, device_id={"mp": mp_peer(k)}, device_id_type=MESH)

    fetches[2].wait()
    fetches[3].wait()
    count = count_ref[0]
    target = expert_ref[...] * CAP + slot_ref[...]
    first = iota((n_dp, rows), 0) * owned
    offset = target - first
    mine = (offset >= 0) & (offset < owned)
    mine_f = mine.astype(F32)
    before = (iota((rows, rows), 0) < iota((rows, rows), 1)).astype(F32).astype(BF16)
    ranks = jnp.dot(mine_f.astype(BF16), before, preferred_element_type=F32)
    rank = jnp.sum(ranks * mine_f, axis=0, keepdims=True)
    base = jnp.sum(iota((n_dp, rows), 0).astype(F32) * mine_f, axis=0, keepdims=True)
    is_live = iota((1, rows), 1) < count
    value = jnp.where(mine & is_live, offset + 1, 0).astype(F32)
    column = (rank + (i * send).astype(F32)).astype(jnp.int32)
    spread = (iota((lanes, rows), 0) == column).astype(F32).astype(BF16)
    table = lax.dot_general(
        value.astype(BF16), spread, (((1,), (1,)), ((), ())), preferred_element_type=F32)
    for o in range(n_dp):
        meta[o, :, :lanes] = table[o:o + 1, :]
        meta[o, :, lanes:] = jnp.full((1, 128), count.astype(F32), F32)
    place = jnp.where(is_live, (base * send + rank).astype(jnp.int32), -1)

    fetches[0].wait()
    fetches[1].wait()
    tokens = tokens_ref[...]
    part[...] = lax.dot_general(
        weight_ref[...], tokens, (((1,), (1,)), ((), ())), preferred_element_type=F32)

    chunk = min(lanes, 256)
    for top in range(0, lanes, chunk):
        pick = (iota((chunk, rows), 0) + top == place).astype(F32).astype(BF16)
        packed[top:top + chunk, :] = jnp.dot(
            pick, tokens, preferred_element_type=F32).astype(BF16)

    pl.semaphore_wait(barrier, n_dp + n_mp - 2)

    def span(index, size):
        return pl.ds(pl.multiple_of(index * size, size), size)

    def p2(peer, at):
        return pltpu.make_async_remote_copy(
            src_ref=part.at[span(peer, share)], dst_ref=part_in.at[at],
            send_sem=p2s.at[peer], recv_sem=p2r.at[at],
            device_id={"mp": peer}, device_id_type=MESH)

    def p3(peer, at):
        block = aff.at[at, span(j, share)]
        return pltpu.make_async_remote_copy(
            src_ref=block, dst_ref=block, send_sem=p3s.at[peer], recv_sem=p3r.at[at],
            device_id={"dp": peer}, device_id_type=MESH)

    pair = j + 1 - 2 * lax.rem(j, 2)

    def direct():
        return [lax.rem(j + 2 * m, n_mp) for m in range(1, n_mp // 2)]

    def p4(peer, at, group, lane=None):
        block = aff.at[group, span(at, share)]
        lane = peer if lane is None else lane
        return pltpu.make_async_remote_copy(
            src_ref=block, dst_ref=block,
            send_sem=p4s.at[lane, group], recv_sem=p4r.at[at, group],
            device_id={"mp": peer}, device_id_type=MESH)

    def bulk(peer, at):
        return pltpu.make_async_remote_copy(
            src_ref=packed.at[span(peer, send)], dst_ref=packed_in.at[span(at, send)],
            send_sem=bs.at[peer], recv_sem=br.at[at],
            device_id={"dp": peer}, device_id_type=MESH)

    def note(peer, at):
        return pltpu.make_async_remote_copy(
            src_ref=meta.at[peer], dst_ref=meta_in.at[at],
            send_sem=ms.at[peer], recv_sem=mr.at[at],
            device_id={"dp": peer}, device_id_type=MESH)

    for k in range(1, n_mp):
        p2(mp_peer(k), j).start()

    split = min(early + 1, n_dp)
    over(1, split, lambda k: bulk(dp_peer(k), i).start())
    over(1, n_dp, lambda k: note(dp_peer(k), i).start())

    total_logits = part[span(j, share), :]
    for k in range(1, n_mp):
        src = mp_peer(k)
        p2(src, src).wait_recv()
        total_logits = total_logits + part_in[src]
    aff[i, span(j, share), :] = jnp.exp(total_logits)
    over(1, n_dp, lambda k: p3(dp_peer(k), i).start())
    for peer in direct() + [pair]:
        p4(peer, j, i).start()
    over(split, n_dp, lambda k: bulk(dp_peer(k), i).start())

    keep = pltpu.make_async_copy(
        packed.at[span(i, send)], packed_in.at[span(i, send)], own.at[4])
    keep.start()
    meta_in[i] = meta[i]

    def forward(k):
        src = lax.rem(i + n_dp - k, n_dp)
        p3(src, src).wait_recv()
        for peer in direct() + [pair]:
            p4(peer, j, src).start()
    over(1, n_dp, forward)

    def across(peer):
        return peer + 1 - 2 * lax.rem(peer, 2)

    def relay(k):
        group = lax.rem(i + n_dp - k, n_dp)
        for src in direct():
            p4(src, src, group).wait_recv()
            p4(pair, src, group, across(src)).start()
    over(0, n_dp, relay)

    over(1, n_dp, lambda k: note(dp_peer(k), dp_peer(k)).wait_recv())
    where_to = jnp.zeros((1, lanes), F32)
    total = jnp.zeros((1, 1), F32)
    for g in range(n_dp):
        value = meta_in[g, :, :lanes]
        where_to = where_to + jnp.where(value > 0, (value - 1) * n_dp + (g + 1), 0.0)
        held = meta_in[g, :, lanes:lanes + 1]
        total = total + held
        live[g] = (iota((1, rows), 1).astype(F32) < held).astype(F32)
    place_ref[...] = (where_to - 1).astype(jnp.int32)

    def landed(k):
        for src in [pair] + [across(peer) for peer in direct()]:
            p4(pair, src, dp_peer(k)).wait_recv()
    over(0, n_dp, landed)

    col_scale = jnp.ones((experts, 1), F32)
    last = col_scale
    for sweep in range(ITERS):
        last = col_scale
        scale = jnp.broadcast_to(last, (experts, rows))

        def add_group(g, acc, scale=scale):
            block = aff[g]
            row_scale = experts / jnp.sum(block * scale, axis=0, keepdims=True)
            return acc + block * (live[g] * row_scale)
        acc = lax.fori_loop(0, n_dp, add_group, jnp.zeros((experts, rows), F32), unroll=few)
        col_scale = total / jnp.sum(acc, axis=1, keepdims=True)

    block = aff[i]
    row_scale = experts / jnp.sum(block * last, axis=0, keepdims=True)
    chosen = expert_ref[...] == iota((experts, rows), 0)
    picked = jnp.sum(jnp.where(chosen, block * col_scale, 0.0), axis=0, keepdims=True)
    gates_ref[...] = live[i] * row_scale * picked

    over(1, n_dp, lambda k: bulk(dp_peer(k), dp_peer(k)).wait_recv())
    keep.wait()

    for k in range(1, n_mp):
        p2(mp_peer(k), j).wait_send()

    def drained(k):
        p3(dp_peer(k), i).wait_send()
        bulk(dp_peer(k), i).wait_send()
        note(dp_peer(k), i).wait_send()
    over(1, n_dp, drained)

    def forwarded(k):
        for peer in direct() + [pair]:
            p4(peer, j, dp_peer(k)).wait_send()
        for src in direct():
            p4(pair, src, dp_peer(k), across(src)).wait_send()
    over(0, n_dp, forwarded)


def unpack(chunk, gates_in, place_ref, packed_ref, gates_ref, out_ref):
    gates_ref[...] = gates_in[...]
    at = iota((chunk, packed_ref.shape[0]), 0) + pl.program_id(0) * chunk
    pick = (at == place_ref[...]).astype(F32).astype(BF16)
    out_ref[...] = jnp.dot(pick, packed_ref[...], preferred_element_type=F32).astype(BF16)


EARLY = 2
CHUNK = 192
VMEM = 67043328
ROOM = 64
SMALL = 16 * 1024 * 1024


def solution(mesh):
    n_dp, n_mp = mesh.shape["dp"], mesh.shape["mp"]

    def local(tokens, router_weight, valid_count, expert_id, slot_id):
        rows, width = tokens.shape
        experts = router_weight.shape[1]
        share = experts // n_mp
        send = -(-(rows // n_dp) // 16) * 16
        lanes = n_dp * send
        slots = experts * CAP // n_dp
        total = slots * n_dp
        chunk = max(c for c in range(16, CHUNK + 1, 16) if total % c == 0)
        limit = VMEM - lanes * width * 2 - ROOM * 1024
        hbm = pl.BlockSpec(memory_space=pltpu.HBM)
        anywhere = pl.BlockSpec(memory_space=pl.ANY)
        vmem = pl.BlockSpec(memory_space=pltpu.VMEM)
        dma = pltpu.SemaphoreType.DMA
        gates, place, packed = pl.pallas_call(
            functools.partial(kernel, n_dp, n_mp, send, EARLY),
            out_shape=(
                pltpu.VMEM((1, rows), F32),
                pltpu.VMEM((1, lanes), jnp.int32),
                pltpu.VMEM((lanes, width), BF16),
            ),
            in_specs=[hbm, hbm, pl.BlockSpec(memory_space=pltpu.SMEM), hbm, hbm],
            out_specs=(vmem, vmem, anywhere),
            scratch_shapes=[
                pltpu.VMEM((rows, width), BF16),
                pltpu.VMEM((experts, width), BF16),
                pltpu.VMEM((1, rows), jnp.int32),
                pltpu.VMEM((1, rows), jnp.int32),
                pltpu.VMEM((experts, rows), F32),
                pltpu.VMEM((n_mp, share, rows), F32),
                pltpu.VMEM((n_dp, experts, rows), F32),
                pltpu.VMEM((lanes, width), BF16),
                pltpu.VMEM((n_dp, 1, lanes + 128), F32),
                pltpu.VMEM((n_dp, 1, lanes + 128), F32),
                pltpu.VMEM((n_dp, 1, rows), F32),
                dma((5,)), dma((n_mp,)), dma((n_mp,)), dma((n_dp,)), dma((n_dp,)),
                dma((n_mp, n_dp)), dma((n_mp, n_dp)),
                dma((n_dp,)), dma((n_dp,)), dma((n_dp,)), dma((n_dp,)),
            ],
            compiler_params=pltpu.CompilerParams(
                collective_id=0, has_side_effects=True, vmem_limit_bytes=limit),
        )(tokens, router_weight.T, valid_count, expert_id.reshape(1, rows), slot_id.reshape(1, rows))
        whole = lambda b: (0, 0)
        gates, out = pl.pallas_call(
            functools.partial(unpack, chunk),
            grid=(total // chunk,),
            out_shape=(
                jax.ShapeDtypeStruct((1, rows), F32),
                jax.ShapeDtypeStruct((total, width), BF16),
            ),
            in_specs=[
                pl.BlockSpec((1, rows), whole), pl.BlockSpec((1, lanes), whole), vmem],
            out_specs=(
                pl.BlockSpec((1, rows), whole), pl.BlockSpec((chunk, width), lambda b: (b, 0))),
            compiler_params=pltpu.CompilerParams(vmem_limit_bytes=SMALL),
        )(gates, place, packed)
        return gates.reshape(rows), out.reshape(slots, n_dp, width)

    placed = (P("dp", "mp"), P("mp", None), P("dp"), P("dp"), P("dp"))
    return jax.shard_map(
        local, mesh=mesh, in_specs=placed, out_specs=(P("dp"), P("dp", None, "mp")), check_vma=False
    )
```
